32 devices in a mesh: pair: 2 (over core), shard: 16 (over z, y, x).
Axes of the slice: x: 2, y: 2, z: 4, core: 2. Of those that a mesh axis runs over, the one named last changes fastest.
Arguments:
- master: float32 [3072, 4096], P('shard', 'pair'), may hold values from -1.5 to 1.5
- gradient: float32 [3072, 4096], P('shard', 'pair'), may hold values from -40 to 40
- first_moment: float32 [3072, 4096], P('shard', 'pair'), may hold values from -4 to 4
- second_moment: float32 [3072, 4096], P('shard', 'pair'), may hold values from 0.02 to 4
- max_norm: float32 [1], replicated, may hold values from 768 to 1536
- step_count: int32 [1], replicated, may hold values from 1 to 1000
Outputs:
- new_master: float32 [3072, 4096], P('shard', 'pair')
- new_first: float32 [3072, 4096], P('shard', 'pair')
- new_second: float32 [3072, 4096], P('shard', 'pair')
- compute_codes: bfloat16 [3072, 4096], P('pair')
- block_scales: bfloat16 [3072, 128], P('pair')
The draws below stay inside these ranges and needn't reach their ends.
All inputs are finite; a program needn't handle non-finite values.
Results may differ from the reference program's by a relative error of at most 0.001.
The reference program's roundings to bfloat16 on the way count: a program that leaves them out, or rounds other values in their place, can miss the bound.
Values may be sent and summed in bfloat16 or wider, within the bound.
A program may use at most 192 MiB of HBM per device.

```python
import math
import jax
import jax.numpy as jnp
from jax import lax

ROWS = 3072
COLS = 4096
BLOCK = 32


def draw_gradient(key, part):
    key_heads, key_halves, key_rows, key_noise = jax.random.split(key, 4)
    head_count = (ROWS + 127) // 128
    head_index = jnp.arange(ROWS) // 128
    head_log = jax.random.uniform(key_heads, (head_count,), minval=-2.0, maxval=2.0)
    head_scale = jnp.exp(head_log)[head_index][:, None]
    half_sign = jnp.where(jax.random.bernoulli(key_halves), 1.0, -1.0)
    upper_half = jnp.arange(COLS) >= COLS // 2
    half_scale = jnp.exp(0.7 * half_sign * jnp.where(upper_half, -1.0, 1.0))[None, :]
    row_scale = jnp.exp(jax.random.uniform(key_rows, (ROWS, 1), minval=-0.7, maxval=0.7))
    noise_part = jnp.clip(jax.random.normal(key_noise, (ROWS, COLS)), -6.0, 6.0)
    values = head_scale * half_scale * row_scale * noise_part
    return jnp.clip(values, -40.0, 40.0).astype(jnp.float32)


def block_scale(key, dims, cuts, low, high):
    def one(axis_at, parts):
        heights = jax.random.uniform(jax.random.fold_in(jax.random.fold_in(key, 6), axis_at), (parts,), jnp.float32, low / len(cuts), high / len(cuts))
        return jnp.repeat(jnp.exp(heights), dims[axis_at] // parts).reshape((-1,) + (1,) * (len(dims) - axis_at - 1))

    gain = one(*cuts[0])
    for cut in cuts[1:]:
        gain = gain * one(*cut)
    return gain


def noise(rng, extent, scale, limit, pieces=(), kind=jnp.bfloat16):
    loudness = block_scale(rng, extent, pieces, -0.22, 0.18) if pieces else 1.0
    drawn = jax.random.normal(rng, extent, jnp.float32) * scale * loudness
    return jnp.minimum(jnp.maximum(drawn, -limit), limit).astype(kind)


def setup_inputs(seed: int = 0) -> dict:
    streams_of = jax.random.split(jax.random.key(seed), 7)
    return {
        "master": noise(streams_of[0], (ROWS, COLS), 0.25, 1.5, ((0, 16), (1, 2)), jnp.float32),
        "gradient": draw_gradient(jax.random.fold_in(streams_of[6], 71), 0),
        "first_moment": noise(streams_of[2], (ROWS, COLS), 0.5, 4.0, ((0, 16), (1, 2)), jnp.float32),
        "second_moment": jnp.clip(jnp.exp(math.log(4.0) - 5.2983174 * jax.random.uniform(streams_of[3], (ROWS, COLS), jnp.float32) ** block_scale(streams_of[3], (ROWS, COLS), ((0, 16), (1, 2)), -0.2, 0.2)), 0.02, 4.0),
        "max_norm": jnp.clip(jax.random.uniform(streams_of[4], (1,), jnp.float32, 768.0, 1536.0), 768.0, 1536.0),
        "step_count": jax.random.randint(streams_of[5], (1,), 1, 1001).astype(jnp.int32),
    }


beta_first = 0.9
beta_second = 0.99
learn_rate = 0.01
decay_rate = 0.1
adam_eps = 1e-06
scale_floor = 0.25

def quantize(weights):
    height, width = weights.shape
    blocked = weights.reshape(height, width // BLOCK, BLOCK)
    largest = lax.optimization_barrier(jnp.max(jnp.abs(blocked), axis=2))
    scales = jnp.maximum(largest, scale_floor).astype(jnp.bfloat16)
    divided = blocked / scales.astype(jnp.float32)[:, :, None]
    return (divided.astype(jnp.bfloat16).reshape(height, width), scales)

def adam_update(master, gradient, first_moment, second_moment, max_norm, step_count, squares):
    norm_limit = max_norm[0]
    clip_factor = norm_limit / jnp.maximum(jnp.sqrt(squares), norm_limit)
    clipped = clip_factor * gradient
    new_first = beta_first * first_moment + (1.0 - beta_first) * clipped
    new_second = beta_second * second_moment + (1.0 - beta_second) * clipped * clipped
    counted = step_count[0].astype(jnp.float32)
    first_fix = 1.0 - jnp.power(jnp.full((), beta_first, jnp.float32), counted)
    second_fix = 1.0 - jnp.power(jnp.full((), beta_second, jnp.float32), counted)
    update = new_first / first_fix / (jnp.sqrt(new_second / second_fix) + adam_eps) + decay_rate * master
    new_master = master - learn_rate * update
    return (new_master, new_first, new_second)

def reference(master, gradient, first_moment, second_moment, max_norm, step_count):
    squares = jnp.sum(gradient * gradient)
    new_master, new_first, new_second = adam_update(master, gradient, first_moment, second_moment, max_norm, step_count, squares)
    compute_codes, block_scales = quantize(new_master)
    return (new_master, new_first, new_second, compute_codes, block_scales)
```

```python
import functools

import jax
import jax.numpy as jnp
from jax import lax
from jax.experimental import pallas as pl
from jax.experimental.pallas import tpu as pltpu
from jax.sharding import PartitionSpec as P

BLOCK = 32
LANES = 128

beta_first = 0.9
beta_second = 0.99
learn_rate = 0.01
decay_rate = 0.1
adam_eps = 1e-06
scale_floor = 0.25

MESH = pl.DeviceIdType.MESH
Z, Y, X = 0, 1, 2
PIECES = (
    ((Z, X, Y), 3),
    ((Z, Y, X), 3),
    ((X, Y, Z), 2),
    ((Z, X, Y), 3),
    ((Z, Y, X), 3),
    ((Y, X, Z), 2),
)
SCALE_ORDER = (Z, X, Y)
WINDOW = 8


def grid_of(mesh):
    count = mesh.shape["shard"]
    at = [d.coords for d in mesh.devices.reshape(mesh.shape["pair"], count)[0]]
    sizes = tuple(len({c[d] for c in at}) for d in (2, 1, 0))
    return sizes


def power(base, exponent):
    result = jnp.float32(1.0)
    for bit in range(31):
        factor = jnp.float32(base ** (2**bit))
        result = jnp.where((exponent >> bit) & 1 == 1, result * factor, result)
    return result


def kernel(
    grid, limit_ref, step_ref, master_hbm, gradient_hbm, first_hbm, second_hbm,
    new_master, new_first, new_second, codes, scales,
    master, gradient, first, second, mine, my_scales, wide_scales, their_scales,
    plane_sums, line_sums,
    load_sem, plane_send, plane_recv, line_send, line_recv,
    own_send, own_scale_send, peer_send, peer_scale_send, peer_scale_recv,
    pass_send, pass_scale_send, code_recv, scale_recv, local_sem,
):
    sizes = grid
    depth, high, wide = sizes
    plane = high * wide
    half_depth = depth // 2
    sources = half_depth * plane
    height, width = mine.shape
    tiles = width // LANES
    core = lax.axis_index("pair")
    chip = lax.axis_index("shard")
    here = (chip // plane, (chip // wide) % high, chip % wide)
    keeper = here[Z] // half_depth
    peer = 1 - core

    def chip_at(at):
        return (at[Z] * high + at[Y]) * wide + at[X]

    loads = [
        pltpu.make_async_copy(source, held, load_sem.at[i])
        for i, (source, held) in enumerate(
            ((gradient_hbm, gradient), (master_hbm, master), (first_hbm, first), (second_hbm, second))
        )
    ]
    for load in loads:
        load.start()

    barrier = pltpu.get_barrier_semaphore()
    group = 2 * plane
    my_place = core * plane + here[Y] * wide + here[X]

    def greet(device):
        pl.semaphore_signal(barrier, inc=1, device_id=device, device_id_type=MESH)

    for place in range(group):
        @pl.when(place != my_place)
        def _():
            greet((place // plane, here[Z] * plane + place % plane))

    for other in range(depth):
        for side in range(2):
            @pl.when(other != here[Z])
            def _():
                greet((side, chip_at((other, here[Y], here[X]))))

    pl.semaphore_wait(barrier, group - 1 + 2 * (depth - 1))

    loads[0].wait()

    def square(i, total):
        rows = gradient[pl.ds(pl.multiple_of(i * 8, 8), 8), :]
        for j in range(tiles):
            part = rows[:, j * LANES : (j + 1) * LANES]
            total = total + part * part
        return total

    total = lax.fori_loop(0, height // 8, square, jnp.zeros((8, LANES), jnp.float32))

    def exchange(value, buffer, place, count, device_of, send_sem, recv_sem):
        buffer[place] = jnp.sum(value, axis=0, keepdims=True)

        def copy(other, slot, sem):
            return pltpu.make_async_remote_copy(
                src_ref=buffer.at[slot], dst_ref=buffer.at[slot],
                send_sem=send_sem.at[other], recv_sem=recv_sem.at[sem],
                device_id=device_of(other), device_id_type=MESH,
            )

        for other in range(count):
            @pl.when(other != place)
            def _():
                copy(other, place, place).start()

        for other in range(count):
            @pl.when(other != place)
            def _():
                copy(other, place, place).wait_send()
                copy(other, other, other).wait_recv()

        return jnp.sum(buffer[...], axis=0)

    total = exchange(
        total, plane_sums, my_place, group,
        lambda place: (place // plane, here[Z] * plane + place % plane), plane_send, plane_recv,
    )
    total = exchange(
        total, line_sums, here[Z], depth,
        lambda other: (core, chip_at((other, here[Y], here[X]))), line_send, line_recv,
    )
    squares = jnp.sum(total, axis=1, keepdims=True)
    norm_limit = jnp.full((1, 1), limit_ref[0], jnp.float32)
    clip_factor = norm_limit / jnp.maximum(jnp.sqrt(squares), norm_limit)
    one = jnp.ones((1, 1), jnp.float32)
    first_gain = one / (one - power(beta_first, step_ref[0]))
    second_gain = one / (one - power(beta_second, step_ref[0]))
    for load in loads[1:]:
        load.wait()

    def children(source, order):
        last = jnp.int32(-1)
        for i, dim in enumerate(order):
            last = jnp.where(here[dim] != source[dim], i, last)
        ways = []
        for i, dim in enumerate(order):
            for side, step in enumerate((1, -1)):
                if sizes[dim] < 2:
                    continue
                there = list(here)
                there[dim] = here[dim] + step
                inside = (there[dim] >= 0) & (there[dim] < sizes[dim])
                away = (here[dim] - source[dim]) * step > 0
                used = inside & ((last < i) | ((last == i) & away))
                ways.append((used, 2 * dim + side, chip_at(there)))
        return ways

    starts = []
    at = 0
    for order, share in PIECES:
        size = tiles * share // sum(s for _, s in PIECES)
        starts.append((at, size))
        at += size
    assert at == tiles

    def code_slice(source, column, k):
        row = (chip_at(source) % sources) * height
        start, size = starts[k]
        lane = column * width + start * LANES
        return codes.at[
            pl.ds(pl.multiple_of(row, 16), height), pl.ds(pl.multiple_of(lane, LANES), size * LANES)
        ]

    def scale_slice(source):
        row = (chip_at(source) % sources) * height
        return scales.at[pl.ds(pl.multiple_of(row, 16), height), :]

    def my_index():
        return chip % sources

    def own_copy(k, send_sem, to):
        start, size = starts[k]
        return pltpu.make_async_remote_copy(
            src_ref=mine.at[:, pl.ds(start * LANES, size * LANES)],
            dst_ref=code_slice(here, core, k),
            send_sem=send_sem, recv_sem=code_recv.at[my_index(), core, k],
            device_id=(keeper, to), device_id_type=MESH,
        )

    def own_local(k):
        start, size = starts[k]
        return pltpu.make_async_copy(
            mine.at[:, pl.ds(start * LANES, size * LANES)], code_slice(here, core, k), local_sem.at[k]
        )

    lane = lax.broadcasted_iota(jnp.int32, (1, LANES), 1)
    pick_row = lax.broadcasted_iota(jnp.int32, (LANES, LANES), 0)
    pick_column = lax.broadcasted_iota(jnp.int32, (LANES, LANES), 1)
    per_tile = LANES // BLOCK
    step_rows = next(r for r in (64, 48, 32, 16) if height % r == 0)

    def tile(i, carry):
        j, r = i // (height // step_rows), i % (height // step_rows)
        rows = pl.ds(pl.multiple_of(r * step_rows, 16), step_rows)
        where = (rows, pl.ds(pl.multiple_of(j * LANES, LANES), LANES))
        weight = master[where]
        clipped = clip_factor * gradient[where]
        moment = beta_first * first[where] + (1.0 - beta_first) * clipped
        power_moment = beta_second * second[where] + (1.0 - beta_second) * clipped * clipped
        new_first[where] = moment
        new_second[where] = power_moment
        update = moment * first_gain / (jnp.sqrt(power_moment * second_gain) + adam_eps)
        weight = weight - learn_rate * (update + decay_rate * weight)
        new_master[where] = weight
        largest = jnp.abs(weight)
        shift = BLOCK // 2
        while shift:
            ahead = pltpu.roll(largest, LANES - shift, axis=1)
            behind = pltpu.roll(largest, shift, axis=1)
            largest = jnp.maximum(largest, jnp.where((lane & shift) == 0, ahead, behind))
            shift //= 2
        scale = jnp.maximum(largest, scale_floor).astype(jnp.bfloat16)
        mine[where] = (weight / scale.astype(jnp.float32)).astype(jnp.bfloat16)
        target = (core * tiles + j) * per_tile + pick_row // BLOCK
        pick = ((pick_row % BLOCK == 0) & (pick_column == target)).astype(jnp.float32)
        wide_scales[rows, :] += jnp.dot(
            scale, pick.astype(jnp.bfloat16), preferred_element_type=jnp.float32
        )
        return carry

    wide_scales[...] = jnp.zeros_like(wide_scales)
    per = height // step_rows
    for k, (order, _) in enumerate(PIECES):
        start, size = starts[k]
        lax.fori_loop(start * per, (start + size) * per, tile, 0)
        for used, way, to in children(here, order):
            @pl.when(used)
            def _():
                own_copy(k, own_send.at[k, way], to).start()

        @pl.when(core == keeper)
        def _():
            own_local(k).start()

        @pl.when(core != keeper)
        def _():
            own_copy(k, peer_send.at[k], chip).start()

    my_scales[...] = wide_scales[...].astype(jnp.bfloat16)
    peer_scales = pltpu.make_async_remote_copy(
        src_ref=my_scales, dst_ref=their_scales, send_sem=peer_scale_send.at[0],
        recv_sem=peer_scale_recv.at[0], device_id=(peer, chip), device_id_type=MESH,
    )

    def scale_copy(source, send_sem, to):
        index = chip_at(source) % sources
        return pltpu.make_async_remote_copy(
            src_ref=scale_slice(source), dst_ref=scale_slice(source),
            send_sem=send_sem, recv_sem=scale_recv.at[index],
            device_id=(core, to), device_id_type=MESH,
        )

    @pl.when(core != keeper)
    def _():
        peer_scales.start()

    @pl.when(core == keeper)
    def _():
        peer_scales.wait_recv()
        merged = wide_scales[...] + their_scales[...].astype(jnp.float32)
        row = pl.ds(pl.multiple_of(my_index() * height, 16), height)
        scales[row, :] = merged.astype(jnp.bfloat16)
        for used, way, to in children(here, SCALE_ORDER):
            @pl.when(used)
            def _():
                scale_copy(here, own_scale_send.at[way], to).start()

    low = core * half_depth
    top = low + half_depth - 1

    def source_of(q):
        i, j = q // plane, q % plane
        inside = low + (here[Z] - low + i + depth) % half_depth
        z = jnp.where(here[Z] >= top, top - i, jnp.where(here[Z] <= low, low + i, inside))
        return (z, (here[Y] + j // wide) % high, (here[X] + j % wide) % wide)

    def code_copy(source, column, k, send_sem, to):
        index = chip_at(source) % sources
        part = code_slice(source, column, k)
        return pltpu.make_async_remote_copy(
            src_ref=part, dst_ref=part, send_sem=send_sem,
            recv_sem=code_recv.at[index, column, k],
            device_id=(core, to), device_id_type=MESH,
        )

    def drain(q):
        source = source_of(q)
        slot = q % WINDOW

        @pl.when(chip_at(source) != chip)
        def _():
            for k, (order, _) in enumerate(PIECES):
                for column in range(2):
                    for used, way, to in children(source, order):
                        @pl.when(used)
                        def _():
                            code_copy(source, column, k, pass_send.at[slot, column, k, way], to).wait_send()

            for used, way, to in children(source, SCALE_ORDER):
                @pl.when(used)
                def _():
                    scale_copy(source, pass_scale_send.at[slot, way], to).wait_send()

    def forward(q, carry):
        source = source_of(q)
        slot = q % WINDOW
        mine_too = chip_at(source) == chip
        if sources > WINDOW:
            @pl.when(q >= WINDOW)
            def _():
                drain(q - WINDOW)

        @pl.when(mine_too)
        def _():
            for k in range(len(PIECES)):
                own_local(k).wait()
                code_copy(source, peer, k, peer_send.at[k], chip).wait_recv()

        @pl.when(jnp.logical_not(mine_too))
        def _():
            for k, (order, _) in enumerate(PIECES):
                ways = children(source, order)
                for column in range(2):
                    code_copy(source, column, k, peer_send.at[k], chip).wait_recv()
                    for used, way, to in ways:
                        @pl.when(used)
                        def _():
                            code_copy(source, column, k, pass_send.at[slot, column, k, way], to).start()

            scale_copy(source, peer_scale_send.at[0], chip).wait_recv()
            for used, way, to in children(source, SCALE_ORDER):
                @pl.when(used)
                def _():
                    scale_copy(source, pass_scale_send.at[slot, way], to).start()

        return carry

    lax.fori_loop(0, sources, forward, 0)

    def drain_step(q, carry):
        drain(q)
        return carry

    lax.fori_loop(max(0, sources - WINDOW), sources, drain_step, 0)
    for k, (order, _) in enumerate(PIECES):
        for used, way, to in children(here, order):
            @pl.when(used)
            def _():
                own_copy(k, own_send.at[k, way], to).wait_send()

        @pl.when(core != keeper)
        def _():
            own_copy(k, peer_send.at[k], chip).wait_send()

    @pl.when(core != keeper)
    def _():
        peer_scales.wait_send()

    @pl.when(core == keeper)
    def _():
        for used, way, to in children(here, SCALE_ORDER):
            @pl.when(used)
            def _():
                scale_copy(here, own_scale_send.at[way], to).wait_send()


def per_device(grid, master, gradient, first_moment, second_moment, max_norm, step_count):
    height, width = master.shape
    plane = grid[1] * grid[2]
    sources = grid[0] * plane // 2
    pieces = len(PIECES)
    kept = sources * height
    state = jax.ShapeDtypeStruct(master.shape, jnp.float32)
    held = pltpu.VMEM(master.shape, jnp.float32)
    narrow = pltpu.VMEM((height, LANES), jnp.bfloat16)
    dma = pltpu.SemaphoreType.DMA
    vmem = pl.BlockSpec(memory_space=pltpu.VMEM)
    smem = pl.BlockSpec(memory_space=pltpu.SMEM)
    hbm = pl.BlockSpec(memory_space=pl.ANY)
    return pl.pallas_call(
        functools.partial(kernel, grid),
        out_shape=(
            pltpu.VMEM(master.shape, jnp.float32),
            pltpu.VMEM(master.shape, jnp.float32),
            pltpu.VMEM(master.shape, jnp.float32),
            pltpu.VMEM((kept, 2 * width), jnp.bfloat16),
            pltpu.VMEM((kept, 2 * width // BLOCK), jnp.bfloat16),
        ) if VMEM_OUT else (
            state, state, state,
            jax.ShapeDtypeStruct((kept, 2 * width), jnp.bfloat16),
            jax.ShapeDtypeStruct((kept, 2 * width // BLOCK), jnp.bfloat16),
        ),
        in_specs=[smem, smem, hbm, hbm, hbm, hbm],
        out_specs=(vmem,) * 5,
        scratch_shapes=[
            held, held, held, held,
            pltpu.VMEM((height, width), jnp.bfloat16),
            narrow,
            pltpu.VMEM((height, LANES), jnp.float32),
            narrow,
            pltpu.VMEM((2 * plane, 1, LANES), jnp.float32),
            pltpu.VMEM((grid[0], 1, LANES), jnp.float32),
            dma((4,)),
            dma((2 * plane,)), dma((2 * plane,)), dma((grid[0],)), dma((grid[0],)),
            dma((pieces, 6)), dma((6,)), dma((pieces,)), dma((1,)), dma((1,)),
            dma((WINDOW, 2, pieces, 6)), dma((WINDOW, 6)),
            dma((sources, 2, pieces)), dma((sources,)), dma((pieces,)),
        ],
        compiler_params=pltpu.CompilerParams(
            collective_id=0, has_side_effects=True, vmem_limit_bytes=KERNEL_VMEM
        ),
    )(max_norm, step_count, master, gradient, first_moment, second_moment)


VMEM_OUT = False
KERNEL_VMEM = 48 * 1024 * 1024


def solution(mesh):
    return jax.shard_map(
        functools.partial(per_device, grid_of(mesh)),
        mesh=mesh,
        in_specs=(
            P("shard", "pair"),
            P("shard", "pair"),
            P("shard", "pair"),
            P("shard", "pair"),
            P(),
            P(),
        ),
        out_specs=(
            P("shard", "pair"),
            P("shard", "pair"),
            P("shard", "pair"),
            P("pair", None),
            P("pair", None),
        ),
        check_vma=False,
    )
```

```python
import functools

import jax
import jax.numpy as jnp
from jax import lax
from jax.experimental import pallas as pl
from jax.experimental.pallas import tpu as pltpu
from jax.sharding import PartitionSpec as P

BLOCK = 32
LANES = 128

beta_first = 0.9
beta_second = 0.99
learn_rate = 0.01
decay_rate = 0.1
adam_eps = 1e-06
scale_floor = 0.25

MESH = pl.DeviceIdType.MESH
Z, Y, X = 0, 1, 2
PIECES = (
    ((Z, X, Y), 3),
    ((Z, Y, X), 3),
    ((X, Y, Z), 2),
    ((Z, X, Y), 3),
    ((Z, Y, X), 3),
    ((Y, X, Z), 2),
)
SCALE_ORDER = (Z, X, Y)
WINDOW = 8


def grid_of(mesh):
    count = mesh.shape["shard"]
    at = [d.coords for d in mesh.devices.reshape(mesh.shape["pair"], count)[0]]
    sizes = tuple(len({c[d] for c in at}) for d in (2, 1, 0))
    return sizes


def power(base, exponent):
    result = jnp.float32(1.0)
    for bit in range(31):
        factor = jnp.float32(base ** (2**bit))
        result = jnp.where((exponent >> bit) & 1 == 1, result * factor, result)
    return result


def kernel(
    grid, limit_ref, step_ref, master_hbm, gradient_hbm, first_hbm, second_hbm,
    new_master, new_first, new_second, codes, scales,
    master, gradient, first, second, mine, my_scales, wide_scales, their_scales,
    plane_sums, line_sums,
    load_sem, plane_send, plane_recv, line_send, line_recv,
    own_send, own_scale_send, peer_send, peer_scale_send, peer_scale_recv,
    pass_send, pass_scale_send, code_recv, scale_recv, local_sem,
):
    sizes = grid
    depth, high, wide = sizes
    plane = high * wide
    half_depth = depth // 2
    sources = half_depth * plane
    height, width = mine.shape
    tiles = width // LANES
    core = lax.axis_index("pair")
    chip = lax.axis_index("shard")
    here = (chip // plane, (chip // wide) % high, chip % wide)
    keeper = here[Z] // half_depth
    peer = 1 - core

    def chip_at(at):
        return (at[Z] * high + at[Y]) * wide + at[X]

    loads = [
        pltpu.make_async_copy(source, held, load_sem.at[i])
        for i, (source, held) in enumerate(
            ((gradient_hbm, gradient), (master_hbm, master), (first_hbm, first), (second_hbm, second))
        )
    ]
    for load in loads:
        load.start()

    barrier = pltpu.get_barrier_semaphore()
    group = 2 * plane
    my_place = core * plane + here[Y] * wide + here[X]

    def greet(device):
        pl.semaphore_signal(barrier, inc=1, device_id=device, device_id_type=MESH)

    for place in range(group):
        @pl.when(place != my_place)
        def _():
            greet((place // plane, here[Z] * plane + place % plane))

    for other in range(depth):
        for side in range(2):
            @pl.when(other != here[Z])
            def _():
                greet((side, chip_at((other, here[Y], here[X]))))

    pl.semaphore_wait(barrier, group - 1 + 2 * (depth - 1))

    loads[0].wait()

    def square(i, total):
        rows = gradient[pl.ds(pl.multiple_of(i * 8, 8), 8), :]
        for j in range(tiles):
            part = rows[:, j * LANES : (j + 1) * LANES]
            total = total + part * part
        return total

    total = lax.fori_loop(0, height // 8, square, jnp.zeros((8, LANES), jnp.float32))

    def exchange(value, buffer, place, count, device_of, send_sem, recv_sem):
        buffer[place] = jnp.sum(value, axis=0, keepdims=True)

        def copy(other, slot, sem):
            return pltpu.make_async_remote_copy(
                src_ref=buffer.at[slot], dst_ref=buffer.at[slot],
                send_sem=send_sem.at[other], recv_sem=recv_sem.at[sem],
                device_id=device_of(other), device_id_type=MESH,
            )

        for other in range(count):
            @pl.when(other != place)
            def _():
                copy(other, place, place).start()

        for other in range(count):
            @pl.when(other != place)
            def _():
                copy(other, place, place).wait_send()
                copy(other, other, other).wait_recv()

        return jnp.sum(buffer[...], axis=0)

    total = exchange(
        total, plane_sums, my_place, group,
        lambda place: (place // plane, here[Z] * plane + place % plane), plane_send, plane_recv,
    )
    total = exchange(
        total, line_sums, here[Z], depth,
        lambda other: (core, chip_at((other, here[Y], here[X]))), line_send, line_recv,
    )
    squares = jnp.sum(total, axis=1, keepdims=True)
    norm_limit = jnp.full((1, 1), limit_ref[0], jnp.float32)
    clip_factor = norm_limit / jnp.maximum(jnp.sqrt(squares), norm_limit)
    one = jnp.ones((1, 1), jnp.float32)
    first_gain = one / (one - power(beta_first, step_ref[0]))
    second_gain = one / (one - power(beta_second, step_ref[0]))
    for load in loads[1:]:
        load.wait()

    def children(source, order):
        last = jnp.int32(-1)
        for i, dim in enumerate(order):
            last = jnp.where(here[dim] != source[dim], i, last)
        ways = []
        for i, dim in enumerate(order):
            for side, step in enumerate((1, -1)):
                if sizes[dim] < 2:
                    continue
                there = list(here)
                there[dim] = here[dim] + step
                inside = (there[dim] >= 0) & (there[dim] < sizes[dim])
                away = (here[dim] - source[dim]) * step > 0
                used = inside & ((last < i) | ((last == i) & away))
                ways.append((used, 2 * dim + side, chip_at(there)))
        return ways

    starts = []
    at = 0
    for order, share in PIECES:
        size = tiles * share // sum(s for _, s in PIECES)
        starts.append((at, size))
        at += size
    assert at == tiles

    def code_slice(source, column, k):
        row = (chip_at(source) % sources) * height
        start, size = starts[k]
        lane = column * width + start * LANES
        return codes.at[
            pl.ds(pl.multiple_of(row, 16), height), pl.ds(pl.multiple_of(lane, LANES), size * LANES)
        ]

    def scale_slice(source):
        row = (chip_at(source) % sources) * height
        return scales.at[pl.ds(pl.multiple_of(row, 16), height), :]

    def my_index():
        return chip % sources

    def own_copy(k, send_sem, to):
        start, size = starts[k]
        return pltpu.make_async_remote_copy(
            src_ref=mine.at[:, pl.ds(start * LANES, size * LANES)],
            dst_ref=code_slice(here, core, k),
            send_sem=send_sem, recv_sem=code_recv.at[my_index(), core, k],
            device_id=(keeper, to), device_id_type=MESH,
        )

    def own_local(k):
        start, size = starts[k]
        return pltpu.make_async_copy(
            mine.at[:, pl.ds(start * LANES, size * LANES)], code_slice(here, core, k), local_sem.at[k]
        )

    lane = lax.broadcasted_iota(jnp.int32, (1, LANES), 1)
    pick_row = lax.broadcasted_iota(jnp.int32, (LANES, LANES), 0)
    pick_column = lax.broadcasted_iota(jnp.int32, (LANES, LANES), 1)
    per_tile = LANES // BLOCK
    step_rows = next(r for r in (64, 48, 32, 16) if height % r == 0)

    def tile(i, carry):
        j, r = i // (height // step_rows), i % (height // step_rows)
        rows = pl.ds(pl.multiple_of(r * step_rows, 16), step_rows)
        where = (rows, pl.ds(pl.multiple_of(j * LANES, LANES), LANES))
        weight = master[where]
        clipped = clip_factor * gradient[where]
        moment = beta_first * first[where] + (1.0 - beta_first) * clipped
        power_moment = beta_second * second[where] + (1.0 - beta_second) * clipped * clipped
        new_first[where] = moment
        new_second[where] = power_moment
        update = moment * first_gain / (jnp.sqrt(power_moment * second_gain) + adam_eps)
        weight = weight - learn_rate * (update + decay_rate * weight)
        new_master[where] = weight
        largest = jnp.abs(weight)
        shift = BLOCK // 2
        while shift:
            ahead = pltpu.roll(largest, LANES - shift, axis=1)
            behind = pltpu.roll(largest, shift, axis=1)
            largest = jnp.maximum(largest, jnp.where((lane & shift) == 0, ahead, behind))
            shift //= 2
        scale = jnp.maximum(largest, scale_floor).astype(jnp.bfloat16)
        mine[where] = (weight / scale.astype(jnp.float32)).astype(jnp.bfloat16)
        target = (core * tiles + j) * per_tile + pick_row // BLOCK
        pick = ((pick_row % BLOCK == 0) & (pick_column == target)).astype(jnp.float32)
        wide_scales[rows, :] += jnp.dot(
            scale, pick.astype(jnp.bfloat16), preferred_element_type=jnp.float32
        )
        return carry

    wide_scales[...] = jnp.zeros_like(wide_scales)
    per = height // step_rows
    for k, (order, _) in enumerate(PIECES):
        start, size = starts[k]
        lax.fori_loop(start * per, (start + size) * per, tile, 0)
        for used, way, to in children(here, order):
            @pl.when(used)
            def _():
                own_copy(k, own_send.at[k, way], to).start()

        @pl.when(core == keeper)
        def _():
            own_local(k).start()

        @pl.when(core != keeper)
        def _():
            own_copy(k, peer_send.at[k], chip).start()

    my_scales[...] = wide_scales[...].astype(jnp.bfloat16)
    peer_scales = pltpu.make_async_remote_copy(
        src_ref=my_scales, dst_ref=their_scales, send_sem=peer_scale_send.at[0],
        recv_sem=peer_scale_recv.at[0], device_id=(peer, chip), device_id_type=MESH,
    )

    def scale_copy(source, send_sem, to):
        index = chip_at(source) % sources
        return pltpu.make_async_remote_copy(
            src_ref=scale_slice(source), dst_ref=scale_slice(source),
            send_sem=send_sem, recv_sem=scale_recv.at[index],
            device_id=(core, to), device_id_type=MESH,
        )

    @pl.when(core != keeper)
    def _():
        peer_scales.start()

    @pl.when(core == keeper)
    def _():
        peer_scales.wait_recv()
        merged = wide_scales[...] + their_scales[...].astype(jnp.float32)
        row = pl.ds(pl.multiple_of(my_index() * height, 16), height)
        scales[row, :] = merged.astype(jnp.bfloat16)
        for used, way, to in children(here, SCALE_ORDER):
            @pl.when(used)
            def _():
                scale_copy(here, own_scale_send.at[way], to).start()

    low = core * half_depth
    top = low + half_depth - 1

    def source_of(q):
        i, j = q // plane, q % plane
        inside = low + (here[Z] - low + i + depth) % half_depth
        z = jnp.where(here[Z] >= top, top - i, jnp.where(here[Z] <= low, low + i, inside))
        return (z, (here[Y] + j // wide) % high, (here[X] + j % wide) % wide)

    def code_copy(source, column, k, send_sem, to):
        index = chip_at(source) % sources
        part = code_slice(source, column, k)
        return pltpu.make_async_remote_copy(
            src_ref=part, dst_ref=part, send_sem=send_sem,
            recv_sem=code_recv.at[index, column, k],
            device_id=(core, to), device_id_type=MESH,
        )

    def drain(q):
        source = source_of(q)
        slot = q % WINDOW

        @pl.when(chip_at(source) != chip)
        def _():
            for k, (order, _) in enumerate(PIECES):
                for column in range(2):
                    for used, way, to in children(source, order):
                        @pl.when(used)
                        def _():
                            code_copy(source, column, k, pass_send.at[slot, column, k, way], to).wait_send()

            for used, way, to in children(source, SCALE_ORDER):
                @pl.when(used)
                def _():
                    scale_copy(source, pass_scale_send.at[slot, way], to).wait_send()

    def forward(q, carry):
        source = source_of(q)
        slot = q % WINDOW
        mine_too = chip_at(source) == chip
        if sources > WINDOW:
            @pl.when(q >= WINDOW)
            def _():
                drain(q - WINDOW)

        @pl.when(mine_too)
        def _():
            for k in range(len(PIECES)):
                own_local(k).wait()
                code_copy(source, peer, k, peer_send.at[k], chip).wait_recv()

        @pl.when(jnp.logical_not(mine_too))
        def _():
            for k, (order, _) in enumerate(PIECES):
                ways = children(source, order)
                for column in range(2):
                    code_copy(source, column, k, peer_send.at[k], chip).wait_recv()
                    for used, way, to in ways:
                        @pl.when(used)
                        def _():
                            code_copy(source, column, k, pass_send.at[slot, column, k, way], to).start()

            scale_copy(source, peer_scale_send.at[0], chip).wait_recv()
            for used, way, to in children(source, SCALE_ORDER):
                @pl.when(used)
                def _():
                    scale_copy(source, pass_scale_send.at[slot, way], to).start()

        return carry

    lax.fori_loop(0, sources, forward, 0)

    def drain_step(q, carry):
        drain(q)
        return carry

    lax.fori_loop(max(0, sources - WINDOW), sources, drain_step, 0)
    for k, (order, _) in enumerate(PIECES):
        for used, way, to in children(here, order):
            @pl.when(used)
            def _():
                own_copy(k, own_send.at[k, way], to).wait_send()

        @pl.when(core != keeper)
        def _():
            own_copy(k, peer_send.at[k], chip).wait_send()

    @pl.when(core != keeper)
    def _():
        peer_scales.wait_send()

    @pl.when(core == keeper)
    def _():
        for used, way, to in children(here, SCALE_ORDER):
            @pl.when(used)
            def _():
                scale_copy(here, own_scale_send.at[way], to).wait_send()


def per_device(grid, master, gradient, first_moment, second_moment, max_norm, step_count):
    height, width = master.shape
    plane = grid[1] * grid[2]
    sources = grid[0] * plane // 2
    pieces = len(PIECES)
    kept = sources * height
    state = jax.ShapeDtypeStruct(master.shape, jnp.float32)
    held = pltpu.VMEM(master.shape, jnp.float32)
    narrow = pltpu.VMEM((height, LANES), jnp.bfloat16)
    dma = pltpu.SemaphoreType.DMA
    vmem = pl.BlockSpec(memory_space=pltpu.VMEM)
    smem = pl.BlockSpec(memory_space=pltpu.SMEM)
    hbm = pl.BlockSpec(memory_space=pltpu.HBM)
    free = pl.BlockSpec(memory_space=pl.ANY)
    state_in = [
        pltpu.with_memory_space_constraint(a, pltpu.HBM)
        for a in (master, gradient, first_moment, second_moment)
    ]
    results = pl.pallas_call(
        functools.partial(kernel, grid),
        out_shape=(
            state, state, state,
            jax.ShapeDtypeStruct((kept, 2 * width), jnp.bfloat16),
            jax.ShapeDtypeStruct((kept, 2 * width // BLOCK), jnp.bfloat16),
        ),
        in_specs=[smem, smem, hbm, hbm, hbm, hbm],
        out_specs=(vmem, vmem, vmem, free, vmem),
        scratch_shapes=[
            held, held, held, held,
            pltpu.VMEM((height, width), jnp.bfloat16),
            narrow,
            pltpu.VMEM((height, LANES), jnp.float32),
            narrow,
            pltpu.VMEM((2 * plane, 1, LANES), jnp.float32),
            pltpu.VMEM((grid[0], 1, LANES), jnp.float32),
            dma((4,)),
            dma((2 * plane,)), dma((2 * plane,)), dma((grid[0],)), dma((grid[0],)),
            dma((pieces, 6)), dma((6,)), dma((pieces,)), dma((1,)), dma((1,)),
            dma((WINDOW, 2, pieces, 6)), dma((WINDOW, 6)),
            dma((sources, 2, pieces)), dma((sources,)), dma((pieces,)),
        ],
        compiler_params=pltpu.CompilerParams(
            collective_id=0, has_side_effects=True, vmem_limit_bytes=KERNEL_VMEM
        ),
    )(max_norm, step_count, *state_in)
    return pl.pallas_call(
        flush,
        out_shape=tuple(jax.ShapeDtypeStruct(r.shape, r.dtype) for r in results),
        in_specs=[free] * len(results),
        out_specs=(hbm,) * len(results),
        scratch_shapes=[dma((len(results), PARTS))],
        compiler_params=pltpu.CompilerParams(vmem_limit_bytes=FLUSH_VMEM),
    )(*results)


def flush(*refs):
    count = len(refs) // 2
    sem = refs[-1]
    copies = []
    for i, (held, out) in enumerate(zip(refs[:count], refs[count:-1])):
        rows = held.shape[0] // PARTS
        for part in range(PARTS):
            span = pl.ds(part * rows, rows)
            copies.append(pltpu.make_async_copy(held.at[span], out.at[span], sem.at[i, part]))
    for copy in copies:
        copy.start()
    for copy in copies:
        copy.wait()


PARTS = 2
FLUSH_VMEM = 1024 * 1024


KERNEL_VMEM = 16 * 1024 * 1024


def solution(mesh):
    return jax.shard_map(
        functools.partial(per_device, grid_of(mesh)),
        mesh=mesh,
        in_specs=(
            P("shard", "pair"),
            P("shard", "pair"),
            P("shard", "pair"),
            P("shard", "pair"),
            P(),
            P(),
        ),
        out_specs=(
            P("shard", "pair"),
            P("shard", "pair"),
            P("shard", "pair"),
            P("pair", None),
            P("pair", None),
        ),
        check_vma=False,
    )
```
